32 devices in a mesh: bucket: 4 (over y, x), seq: 8 (over z, core).
Axes of the slice: x: 2, y: 2, z: 4, core: 2. Of those that a mesh axis runs over, the one named last changes fastest.
Arguments:
- queries: bfloat16 [4, 448, 1536], P('bucket', 'seq'), may hold values from -45 to 45, as said below
- keys: bfloat16 [4, 448, 1536], P('bucket', 'seq'), may hold values from -5 to 5
- values: bfloat16 [4, 448, 1536], P('bucket', 'seq'), may hold values from -6 to 6
- bucket_lens: int32 [4], P('bucket'), may hold values from 224 to 392
- gate: float32 [4, 3072], P('bucket'), may hold values from 0.5 to 2
- out_weight: bfloat16 [1536, 3072], P(None, 'bucket'), may hold values from -0.15625 to 0.15625
Outputs:
- gated_out: bfloat16 [4, 448, 3072], P('bucket', 'seq')
The draws below stay inside these ranges and needn't reach their ends.
Inputs may be any that keep to these rules, and one draw needn't show every extreme that they name: queries of a few tokens in a bucket may be strong multiples of some keys.
All inputs are finite; a program needn't handle non-finite values.
Results may differ from the reference program's by a relative error of at most 0.013.
Values may be sent and summed in bfloat16 or wider, within the bound.
A program may use at most 192 MiB of HBM per device.

```python
import jax
import jax.numpy as jnp
from jax import lax

D = 3072
HEADS = 12
HEAD_DIM = 128
TOK_DEV = 56
BUCKETS = 4
TOKENS = 448


def query_key_pair(key):
    base = jax.random.fold_in(key, 7)
    key_q, key_k = jax.random.split(base, 2)
    shape = (BUCKETS, TOKENS, HEADS * HEAD_DIM)
    queries = jnp.clip(1.6 * jax.random.normal(key_q, shape, jnp.float32), -5.0, 5.0)
    keys = jnp.clip(1.6 * jax.random.normal(key_k, shape, jnp.float32), -5.0, 5.0)
    return (queries, keys)


def draw_queries(key, part):
    return query_key_pair(key)[0].astype(jnp.bfloat16)


def draw_keys(key, part):
    return query_key_pair(key)[1].astype(jnp.bfloat16)


def with_ends(entries, stream_key, smallest, largest):
    longest = entries.shape.index(max(entries.shape))
    spots = []
    for shift in (0, 1):
        where = [jax.random.randint(jax.random.fold_in(stream_key, axis), (), 0, length) for axis, length in enumerate(entries.shape)]
        where[longest] = (where[longest] + shift) % entries.shape[longest]
        spots.append(tuple(where))
    return entries.at[spots[0]].set(smallest).at[spots[1]].set(largest)


def shard_levels(key, shape, pieces, low, high):
    loudness, own = 1.0, jax.random.fold_in(key, 6)
    for dim, blocks in pieces:
        steps = jnp.exp(jax.random.uniform(jax.random.fold_in(own, dim), (blocks,), jnp.float32, low / len(pieces), high / len(pieces)))
        loudness = loudness * jnp.repeat(steps, shape[dim] // blocks).reshape([-1 if axis == dim else 1 for axis in range(len(shape))])
    return loudness


def gaussian(own_key, dims, spread, limit, pieces=(), kind=jnp.bfloat16):
    array = jax.random.normal(own_key, dims, jnp.float32) * spread
    if len(pieces) > 0:
        array = shard_levels(own_key, dims, pieces, -0.22, 0.18) * array
    return jnp.clip(array, min=-limit, max=limit).astype(kind)


def setup_inputs(seed: int = 0) -> dict:
    streams_of = jax.random.split(jax.random.key(seed), 7)
    queries = draw_queries(jax.random.fold_in(streams_of[6], 71), 0)
    keys = draw_keys(jax.random.fold_in(streams_of[6], 71), 0)
    values = gaussian(streams_of[2], (BUCKETS, TOKENS, HEADS * HEAD_DIM), 1.0, 6.0, ((0, 4), (1, 8)))
    bucket_lens = with_ends(jax.random.randint(streams_of[3], (BUCKETS,), TOKENS // 2, TOKENS - TOK_DEV + 1), jax.random.fold_in(streams_of[3], 1), TOKENS // 2, TOKENS - TOK_DEV).astype(jnp.int32)
    gate = jnp.clip(0.5 + 1.5 * jax.random.uniform(streams_of[4], (BUCKETS, D), jnp.float32) ** shard_levels(streams_of[4], (BUCKETS, D), ((0, 4),), -0.2, 0.2), 0.5, 2.0)
    out_weight = gaussian(streams_of[5], (HEADS * HEAD_DIM, D), (HEADS * HEAD_DIM) ** -0.5, 0.15625, ((1, 4),))
    return dict(queries=queries, keys=keys, values=values, bucket_lens=bucket_lens, gate=gate, out_weight=out_weight)


NEG_FILL = -1.0e30


def block_stats(queries, keys, values, usable):
    scores = jnp.einsum("qhe,nkhe->nhqk", queries, keys) * (HEAD_DIM ** -0.5)
    keep_mask = usable[:, None, None, :]
    scores = jnp.where(keep_mask, scores, NEG_FILL)
    maxima = jnp.max(scores, axis=3)
    weights = jnp.where(keep_mask, jnp.exp(scores - maxima[..., None]), 0.0)
    totals = jnp.sum(weights, axis=3)
    rounded = lax.optimization_barrier(weights.astype(jnp.bfloat16)).astype(jnp.float32)
    weighted = jnp.einsum("nhqk,nkhe->nqhe", rounded, values)
    divisor = jnp.transpose(jnp.maximum(totals, 1.0), (0, 2, 1))
    partial_value = (weighted / divisor[..., None]).astype(jnp.bfloat16)
    return partial_value, jnp.transpose(maxima, (0, 2, 1)), jnp.transpose(totals, (0, 2, 1))


def combine(partial_value, maxima, totals):
    row_max = jnp.max(maxima, axis=0)
    factors = totals * jnp.exp(maxima - row_max[None])
    partial_wide = lax.optimization_barrier(partial_value).astype(jnp.float32)
    summed = jnp.einsum("nqh,nqhe->qhe", factors, partial_wide)
    attended = summed / jnp.sum(factors, axis=0)[..., None]
    return attended.reshape(attended.shape[0], -1).astype(jnp.bfloat16)


def reference(queries, keys, values, bucket_lens, gate, out_weight):
    count = queries.shape[1]
    block_count = count // TOK_DEV
    positions = jnp.arange(count, dtype=jnp.int32)
    results = []
    for bucket in range(queries.shape[0]):
        length = bucket_lens[bucket]
        key_blocks = keys[bucket].astype(jnp.float32).reshape(block_count, TOK_DEV, HEADS, HEAD_DIM)
        value_blocks = values[bucket].astype(jnp.float32).reshape(block_count, TOK_DEV, HEADS, HEAD_DIM)
        usable = (positions < length).reshape(block_count, TOK_DEV)
        query_blocks = queries[bucket].reshape(block_count, TOK_DEV, HEADS, HEAD_DIM)

        def one_block(query_block):
            partial_value, maxima, totals = block_stats(query_block.astype(jnp.float32), key_blocks, value_blocks, usable)
            return combine(partial_value, maxima, totals)

        attended = lax.map(one_block, query_blocks).reshape(count, HEADS * HEAD_DIM)
        projected = jnp.dot(attended, out_weight, preferred_element_type=jnp.float32) * gate[bucket][None, :]
        projected = jnp.where((positions < length)[:, None], projected, 0.0)
        results.append(projected.astype(jnp.bfloat16))
    return jnp.stack(results)
```

```python
import functools

import jax
import jax.numpy as jnp
from jax import lax
from jax.experimental import pallas as pl
from jax.experimental.pallas import tpu as pltpu
from jax.sharding import PartitionSpec as P

HEADS = 12
HEAD_DIM = 128
CORES = 2

NEG_FILL = -1e30


def block_stats(queries, keys, values, usable):
    scores = jnp.einsum(
        "qhe,nkhe->nhqk", queries, keys, preferred_element_type=jnp.float32
    ) * HEAD_DIM ** (-0.5)
    keep_mask = usable[:, None, None, :]
    scores = jnp.where(keep_mask, scores, NEG_FILL)
    maxima = jnp.max(scores, axis=3)
    weights = jnp.where(keep_mask, jnp.exp(scores - maxima[..., None]), 0.0)
    totals = jnp.sum(weights, axis=3)
    weighted = jnp.einsum(
        "nhqk,nkhe->nqhe", weights.astype(jnp.bfloat16), values, preferred_element_type=jnp.float32
    )
    divisor = jnp.transpose(jnp.maximum(totals, 1.0), (0, 2, 1))
    partial_value = (weighted / divisor[..., None]).astype(jnp.bfloat16)
    return (partial_value, jnp.transpose(maxima, (0, 2, 1)), jnp.transpose(totals, (0, 2, 1)))


def combine(partial_value, maxima, totals):
    row_max = jnp.max(maxima, axis=0)
    factors = totals * jnp.exp(maxima - row_max[None])
    summed = jnp.einsum("nqh,nqhe->qhe", factors, partial_value.astype(jnp.float32))
    attended = summed / jnp.sum(factors, axis=0)[..., None]
    return attended.reshape(attended.shape[0], -1).astype(jnp.bfloat16)


def shards(queries, keys, values, bucket_lens, gate, out_weight):
    rows_here = queries.shape[1]
    width = queries.shape[2]
    length = bucket_lens[0]
    position = lax.axis_index("seq") * rows_here + lax.iota(jnp.int32, rows_here)
    queries_all = lax.all_gather(queries[0], "seq", axis=0, tiled=True)
    count_all = queries_all.shape[0]
    key_usable = (position < length)[None, :]
    partial_value, maxima, totals = block_stats(
        queries_all.reshape(count_all, HEADS, HEAD_DIM),
        keys[0].reshape(1, rows_here, HEADS, HEAD_DIM),
        values[0].reshape(1, rows_here, HEADS, HEAD_DIM),
        key_usable,
    )
    block_max, block_total = (
        lax.all_to_all(maxima, "seq", split_axis=1, concat_axis=0, tiled=True),
        lax.all_to_all(totals, "seq", split_axis=1, concat_axis=0, tiled=True),
    )
    block_part = lax.all_to_all(
        partial_value.reshape(1, count_all, width), "seq", split_axis=1, concat_axis=0, tiled=True
    )
    shaped = block_part.reshape(block_part.shape[0], block_part.shape[1], HEADS, HEAD_DIM)
    attended = combine(shaped, block_max, block_total)
    gate_row = gate[0]
    projected = (
        jnp.dot(
            attended,
            lax.all_gather(out_weight, "bucket", axis=1, tiled=True),
            preferred_element_type=jnp.float32,
        )
        * gate_row[None, :]
    )
    result = jnp.where((position < length)[:, None], projected, 0.0).astype(jnp.bfloat16)
    return result[None]


def remote(src, dst, send, recv, where):
    return pltpu.make_async_remote_copy(
        src_ref=src, dst_ref=dst, send_sem=send, recv_sem=recv,
        device_id=where, device_id_type=pl.DeviceIdType.MESH,
    )


def stack_rows(blocks):
    wide = jnp.concatenate([block.astype(jnp.float32) for block in blocks], axis=0)
    return wide.astype(jnp.bfloat16)


def fused_kernel(
    nb, nz, len_ref, q_hbm, k_hbm, v_hbm, w_hbm, out_ref,
    own, weight, qbuf, kvbuf, att, xbuf, ybuf,
    load_sem, slot_sem, w_sem, a_send, a_recv, c_send, c_recv,
    r_send, r_recv, m_send, m_recv, y_send, y_recv,
):
    rows = qbuf.shape[1]
    span = qbuf.shape[2]
    cols = weight.shape[1]
    bucket = lax.axis_index("bucket")
    seq = lax.axis_index("seq")
    z = seq // CORES
    core = lax.rem(seq, CORES)
    steps = [1, nz - 1] + list(range(2, nz - 1)) if nz > 2 else list(range(1, nz))
    others = [lax.rem(z + step, nz) for step in steps]
    peers = [lax.rem(bucket + step, nb) for step in range(1, nb)]
    partner = (bucket, z * CORES + (1 - core))

    def chip(other):
        return (bucket, other * CORES + core)

    loads = []
    for kind, ref in ((1, k_hbm), (0, q_hbm), (2, v_hbm)):
        copy = pltpu.make_async_copy(ref.at[0], own.at[kind], load_sem.at[kind])
        copy.start()
        loads.append(copy)
    columns = pl.ds(pl.multiple_of(z * span, 128), span)
    slots = [
        pltpu.make_async_copy(q_hbm.at[0, :, columns], qbuf.at[z], slot_sem.at[0]),
        pltpu.make_async_copy(k_hbm.at[0, :, columns], kvbuf.at[0, seq], slot_sem.at[1]),
        pltpu.make_async_copy(v_hbm.at[0, :, columns], kvbuf.at[1, seq], slot_sem.at[2]),
    ]
    for copy in slots:
        copy.start()
    w_copy = pltpu.make_async_copy(w_hbm, weight, w_sem)
    w_copy.start()

    barrier = pltpu.get_barrier_semaphore()
    friends = [partner] + [chip(o) for o in others] + [(p, seq) for p in peers]
    for friend in friends:
        pl.semaphore_signal(
            barrier, inc=1, device_id=friend, device_id_type=pl.DeviceIdType.MESH
        )
    for copy in loads + slots:
        copy.wait()
    pl.semaphore_wait(barrier, len(friends))

    pending = []
    for kind in (1, 0, 2):
        for other in others:
            part = own.at[kind, :, pl.ds(pl.multiple_of(other * span, 128), span)]
            target = qbuf.at[z] if kind == 0 else kvbuf.at[kind - 1, seq]
            copy = remote(
                part, target, a_send.at[kind, other], a_recv.at[kind, z], chip(other)
            )
            copy.start()
            pending.append(copy)

    def arrived(kind, other):
        place = qbuf.at[other] if kind == 0 else kvbuf.at[kind - 1, other * CORES + core]
        remote(place, place, a_send.at[kind, other], a_recv.at[kind, other], partner).wait_recv()

    def share(kind, other):
        place = kvbuf.at[kind - 1, other * CORES + core]
        copy = remote(
            place, place, c_send.at[kind - 1, other], c_recv.at[kind - 1, other], partner
        )
        copy.start()
        pending.append(copy)

    def shared(kind):
        for other in range(nz):
            place = kvbuf.at[kind - 1, other * CORES + (1 - core)]
            remote(
                place, place, c_send.at[kind - 1, other], c_recv.at[kind - 1, other], partner
            ).wait_recv()

    share(1, z)
    share(2, z)
    for other in others:
        arrived(1, other)
        share(1, other)
    for other in others:
        arrived(0, other)
    shared(1)
    for other in others:
        arrived(2, other)
        share(2, other)

    length = len_ref[0]
    heads = span // HEAD_DIM
    blocks = nz * CORES
    query_all = stack_rows([qbuf[i] for i in range(nz)])
    key_all = stack_rows([kvbuf[0, j] for j in range(blocks)])
    usable = lax.broadcasted_iota(jnp.int32, (blocks * rows, nz * rows), 0) < length
    probs = []
    sums = []
    for h in range(heads):
        lanes = slice(h * HEAD_DIM, (h + 1) * HEAD_DIM)
        scores = lax.dot_general(
            key_all[:, lanes], query_all[:, lanes], (((1,), (1,)), ((), ())),
            preferred_element_type=jnp.float32,
        ) * HEAD_DIM ** (-0.5)
        scores = jnp.where(usable, scores, NEG_FILL)
        top = jnp.max(scores, axis=0, keepdims=True)
        prob = jnp.exp(scores - top)
        sums.append(jnp.sum(prob, axis=0, keepdims=True))
        probs.append(prob.astype(jnp.bfloat16))
    shared(2)
    value_all = stack_rows([kvbuf[1, j] for j in range(blocks)])
    lane = lax.broadcasted_iota(jnp.int32, (1, nz * rows), 1)
    token = lane + (lane // rows) * ((CORES - 1) * rows) + core * rows
    for h in range(heads):
        lanes = slice(h * HEAD_DIM, (h + 1) * HEAD_DIM)
        summed = lax.dot_general(
            value_all[:, lanes], probs[h], (((0,), (0,)), ((), ())),
            preferred_element_type=jnp.float32,
        )
        normal = jnp.where(token < length, summed / sums[h], 0.0).T
        for i in range(nz):
            att[i, :, lanes] = normal[i * rows:(i + 1) * rows].astype(jnp.bfloat16)

    for other in others:
        copy = remote(
            att.at[other], xbuf.at[bucket, z], r_send.at[other], r_recv.at[z], chip(other)
        )
        copy.start()
        pending.append(copy)
    xbuf[bucket, z] = att[z]

    def spread(source, other):
        for peer in peers:
            copy = remote(
                source, xbuf.at[bucket, other],
                m_send.at[peer, other], m_recv.at[bucket, other], (peer, seq),
            )
            copy.start()
            pending.append(copy)

    spread(att.at[z], z)
    for other in others:
        place = xbuf.at[bucket, other]
        remote(place, place, r_send.at[other], r_recv.at[other], partner).wait_recv()
        spread(place, other)

    w_copy.wait()
    here = pl.ds(pl.multiple_of(bucket * cols, 128), cols)

    def project(which):
        left = jnp.concatenate([xbuf[which, i] for i in range(nz)], axis=1)
        return jnp.dot(left, weight[...], preferred_element_type=jnp.float32).astype(jnp.bfloat16)

    out_ref[:, here] = project(bucket)
    for peer in peers:
        for other in range(nz):
            place = xbuf.at[peer, other]
            remote(
                place, place, m_send.at[peer, other], m_recv.at[peer, other], partner
            ).wait_recv()
        ybuf[peer] = project(peer)
        copy = remote(
            ybuf.at[peer], out_ref.at[:, here], y_send.at[peer], y_recv.at[bucket], (peer, seq)
        )
        copy.start()
        pending.append(copy)
    for peer in peers:
        place = out_ref.at[:, pl.ds(pl.multiple_of(peer * cols, 128), cols)]
        remote(ybuf.at[peer], place, y_send.at[peer], y_recv.at[peer], partner).wait_recv()
    for copy in pending:
        copy.wait_send()


def fused_shards(nb, nz, queries, keys, values, bucket_lens, gate, out_weight):
    rows, width = queries.shape[1:]
    cols = out_weight.shape[1]
    span = width // nz
    low = jnp.bfloat16
    dma = pltpu.SemaphoreType.DMA
    anywhere = pl.BlockSpec(memory_space=pl.ANY)
    projected = pl.pallas_call(
        functools.partial(fused_kernel, nb, nz),
        out_shape=jax.ShapeDtypeStruct((rows, nb * cols), low),
        in_specs=[pl.BlockSpec(memory_space=pltpu.SMEM)] + [anywhere] * 4,
        out_specs=pl.BlockSpec(memory_space=pltpu.VMEM),
        scratch_shapes=[
            pltpu.VMEM((3, rows, width), low),
            pltpu.VMEM((width, cols), low),
            pltpu.VMEM((nz, rows, span), low),
            pltpu.VMEM((2, nz * CORES, rows, span), low),
            pltpu.VMEM((nz, rows, span), low),
            pltpu.VMEM((nb, nz, rows, span), low),
            pltpu.VMEM((nb, rows, cols), low),
            dma((3,)), dma((3,)), dma,
            dma((3, nz)), dma((3, nz)),
            dma((2, nz)), dma((2, nz)),
            dma((nz,)), dma((nz,)),
            dma((nb, nz)), dma((nb, nz)),
            dma((nb,)), dma((nb,)),
        ],
        compiler_params=pltpu.CompilerParams(collective_id=0, has_side_effects=True),
    )(bucket_lens, queries, keys, values, out_weight)
    position = lax.axis_index("seq") * rows + lax.iota(jnp.int32, rows)
    gated = projected.astype(jnp.float32) * gate[0][None, :]
    keep = (position < bucket_lens[0])[:, None]
    return jnp.where(keep, gated, 0.0).astype(jnp.bfloat16)[None]


def solution(mesh):
    placed = (
        P("bucket", "seq", None),
        P("bucket", "seq", None),
        P("bucket", "seq", None),
        P("bucket"),
        P("bucket", None),
        P(None, "bucket"),
    )
    nb, ns = mesh.shape["bucket"], mesh.shape["seq"]
    body = shards
    if ns % CORES == 0 and HEADS % (ns // CORES) == 0:
        body = functools.partial(fused_shards, nb, ns // CORES)
    return jax.shard_map(
        body, mesh=mesh, in_specs=placed, out_specs=P("bucket", "seq", None), check_vma=False
    )
```

```python
import functools

import jax
import jax.numpy as jnp
from jax import lax
from jax.experimental import pallas as pl
from jax.experimental.pallas import tpu as pltpu
from jax.sharding import PartitionSpec as P

HEADS = 12
HEAD_DIM = 128
CORES = 2
CHUNKS = 2

NEG_FILL = -1e30


def block_stats(queries, keys, values, usable):
    scores = jnp.einsum(
        "qhe,nkhe->nhqk", queries, keys, preferred_element_type=jnp.float32
    ) * HEAD_DIM ** (-0.5)
    keep_mask = usable[:, None, None, :]
    scores = jnp.where(keep_mask, scores, NEG_FILL)
    maxima = jnp.max(scores, axis=3)
    weights = jnp.where(keep_mask, jnp.exp(scores - maxima[..., None]), 0.0)
    totals = jnp.sum(weights, axis=3)
    weighted = jnp.einsum(
        "nhqk,nkhe->nqhe", weights.astype(jnp.bfloat16), values, preferred_element_type=jnp.float32
    )
    divisor = jnp.transpose(jnp.maximum(totals, 1.0), (0, 2, 1))
    partial_value = (weighted / divisor[..., None]).astype(jnp.bfloat16)
    return (partial_value, jnp.transpose(maxima, (0, 2, 1)), jnp.transpose(totals, (0, 2, 1)))


def combine(partial_value, maxima, totals):
    row_max = jnp.max(maxima, axis=0)
    factors = totals * jnp.exp(maxima - row_max[None])
    summed = jnp.einsum("nqh,nqhe->qhe", factors, partial_value.astype(jnp.float32))
    attended = summed / jnp.sum(factors, axis=0)[..., None]
    return attended.reshape(attended.shape[0], -1).astype(jnp.bfloat16)


def shards(queries, keys, values, bucket_lens, gate, out_weight):
    rows_here = queries.shape[1]
    width = queries.shape[2]
    length = bucket_lens[0]
    position = lax.axis_index("seq") * rows_here + lax.iota(jnp.int32, rows_here)
    queries_all = lax.all_gather(queries[0], "seq", axis=0, tiled=True)
    count_all = queries_all.shape[0]
    key_usable = (position < length)[None, :]
    partial_value, maxima, totals = block_stats(
        queries_all.reshape(count_all, HEADS, HEAD_DIM),
        keys[0].reshape(1, rows_here, HEADS, HEAD_DIM),
        values[0].reshape(1, rows_here, HEADS, HEAD_DIM),
        key_usable,
    )
    block_max, block_total = (
        lax.all_to_all(maxima, "seq", split_axis=1, concat_axis=0, tiled=True),
        lax.all_to_all(totals, "seq", split_axis=1, concat_axis=0, tiled=True),
    )
    block_part = lax.all_to_all(
        partial_value.reshape(1, count_all, width), "seq", split_axis=1, concat_axis=0, tiled=True
    )
    shaped = block_part.reshape(block_part.shape[0], block_part.shape[1], HEADS, HEAD_DIM)
    attended = combine(shaped, block_max, block_total)
    gate_row = gate[0]
    projected = (
        jnp.dot(
            attended,
            lax.all_gather(out_weight, "bucket", axis=1, tiled=True),
            preferred_element_type=jnp.float32,
        )
        * gate_row[None, :]
    )
    result = jnp.where((position < length)[:, None], projected, 0.0).astype(jnp.bfloat16)
    return result[None]


def remote(src, dst, send, recv, where):
    return pltpu.make_async_remote_copy(
        src_ref=src, dst_ref=dst, send_sem=send, recv_sem=recv,
        device_id=where, device_id_type=pl.DeviceIdType.MESH,
    )


def stack_rows(blocks):
    wide = jnp.concatenate([block.astype(jnp.float32) for block in blocks], axis=0)
    return wide.astype(jnp.bfloat16)


def row_chunks(rows):
    if CHUNKS == 1 or rows % 8 != 0 or rows < 32:
        return [(0, rows)]
    head = (rows // 2 + 15) // 16 * 16
    return [(0, head), (head, rows - head)]


def fused_kernel(nb, nz, chunks, len_ref, q_hbm, k_hbm, v_hbm, w_hbm, out_ref, *refs):
    (
        own, weight, kvbuf, load_sem, slot_sem, w_sem, a_send, a_recv, q_send, q_recv,
        c_send, c_recv, r_send, r_recv, m_send, m_recv, y_send, y_recv,
    ) = refs[:18]
    count = len(chunks)
    qbufs, atts, xbufs, ybufs = [refs[18 + n * count:18 + (n + 1) * count] for n in range(4)]
    _, _, rows, span = kvbuf.shape
    cols = weight.shape[1]
    bucket = lax.axis_index("bucket")
    seq = lax.axis_index("seq")
    z = seq // CORES
    core = lax.rem(seq, CORES)
    last = nz * CORES - 1
    alive = seq < last
    steps = [1, nz - 1] + list(range(2, nz - 1)) if nz > 2 else list(range(1, nz))
    others = [lax.rem(z + step, nz) for step in steps]
    peers = [lax.rem(bucket + step, nb) for step in range(1, nb)]
    if nb & (nb - 1) == 0:
        peers = [lax.bitwise_xor(bucket, step) for step in range(1, nb)]
    partner = (bucket, z * CORES + (1 - core))

    def chip(other):
        return (bucket, other * CORES + core)

    def holds(other, which):
        return other * CORES + which < last

    barrier = pltpu.get_barrier_semaphore()
    friends = [chip(o) for o in reversed(others)] + [(p, seq) for p in peers] + [partner]
    for friend in friends:
        pl.semaphore_signal(
            barrier, inc=1, device_id=friend, device_id_type=pl.DeviceIdType.MESH
        )

    loads = []
    for kind, ref in ((1, k_hbm), (0, q_hbm), (2, v_hbm)):
        loads.append(pltpu.make_async_copy(ref.at[0], own.at[kind], load_sem.at[kind]))
    mine = pl.ds(pl.multiple_of(z * span, 128), span)
    for kind, ref in ((0, k_hbm), (1, v_hbm)):
        loads.append(
            pltpu.make_async_copy(ref.at[0, :, mine], kvbuf.at[kind, seq], slot_sem.at[kind])
        )
    for copy in loads:
        copy.start()
    w_copy = pltpu.make_async_copy(w_hbm, weight, w_sem)
    w_copy.start()
    for copy in loads:
        copy.wait()
    pl.semaphore_wait(barrier, len(friends))

    def lanes_of(other):
        return pl.ds(pl.multiple_of(other * span, 128), span)

    def send_keys(kind, other):
        return remote(
            own.at[1 + kind, :, lanes_of(other)], kvbuf.at[kind, seq],
            a_send.at[kind, other], a_recv.at[kind, z], chip(other),
        )

    def send_queries(c, other):
        start, size = chunks[c]
        return remote(
            own.at[0, pl.ds(start, size), lanes_of(other)], qbufs[c].at[z],
            q_send.at[c, other], q_recv.at[c, z], chip(other),
        )

    def share(kind, other, which):
        place = kvbuf.at[kind, other * CORES + which]
        return remote(
            place, place, c_send.at[kind, other], c_recv.at[kind, other], partner
        )

    def back(c, other):
        return remote(
            atts[c].at[other], xbufs[c].at[bucket, z], r_send.at[c, other], r_recv.at[c, z],
            chip(other),
        )

    def spread(c, other, peer, source):
        return remote(
            source, xbufs[c].at[bucket, other],
            m_send.at[c, peer, other], m_recv.at[c, bucket, other], (peer, seq),
        )

    def columns_of(which):
        return pl.ds(pl.multiple_of(which * cols, 128), cols)

    def result(c, peer, which):
        place = out_ref.at[pl.ds(*chunks[c]), columns_of(which)]
        return remote(
            ybufs[c].at[peer], place, y_send.at[c, peer], y_recv.at[c, which], (peer, seq)
        )

    @pl.when(alive)
    def _():
        for other in others:
            send_keys(0, other).start()
        for other in others:
            send_queries(0, other).start()
        for other in others:
            send_keys(1, other).start()
        for c in range(1, count):
            for other in others:
                send_queries(c, other).start()
        share(0, z, core).start()
        share(1, z, core).start()

    for c, (start, size) in enumerate(chunks):
        qbufs[c][z] = own[0, start:start + size, mine]

    def take_keys(kind):
        for other in others:
            @pl.when(holds(other, core))
            def _():
                place = kvbuf.at[kind, other * CORES + core]
                remote(
                    place, place, a_send.at[kind, other], a_recv.at[kind, other], partner
                ).wait_recv()
                share(kind, other, core).start()

    def take_shared(kind):
        for other in range(nz):
            @pl.when(holds(other, 1 - core))
            def _():
                share(kind, other, 1 - core).wait_recv()

    def take_queries(c):
        for other in others:
            @pl.when(holds(other, core))
            def _():
                place = qbufs[c].at[other]
                remote(
                    place, place, q_send.at[c, other], q_recv.at[c, other], partner
                ).wait_recv()

    length = len_ref[0]
    heads = [slice(h * HEAD_DIM, (h + 1) * HEAD_DIM) for h in range(span // HEAD_DIM)]

    def weigh(c, key_all):
        size = chunks[c][1]
        query_all = stack_rows([qbufs[c][i] for i in range(nz)])
        usable = lax.broadcasted_iota(jnp.int32, (last * rows, nz * size), 0) < length
        probs = []
        for lanes in heads:
            scores = lax.dot_general(
                key_all[:, lanes], query_all[:, lanes], (((1,), (1,)), ((), ())),
                preferred_element_type=jnp.float32,
            ) * HEAD_DIM ** (-0.5)
            scores = jnp.where(usable, scores, NEG_FILL)
            top = jnp.max(scores, axis=0, keepdims=True)
            prob = jnp.exp(scores - top)
            probs.append((prob.astype(jnp.bfloat16), jnp.sum(prob, axis=0, keepdims=True)))
        return probs

    def attend(c, probs, value_all):
        start, size = chunks[c]
        lane = lax.broadcasted_iota(jnp.int32, (1, nz * size), 1)
        block = lane // size
        token = (block * CORES + core) * rows + start + (lane - block * size)
        for lanes, (prob, total) in zip(heads, probs):
            summed = lax.dot_general(
                value_all[:, lanes], prob, (((0,), (0,)), ((), ())),
                preferred_element_type=jnp.float32,
            )
            normal = jnp.where(token < length, summed / total, 0.0).T
            for i in range(nz):
                atts[c][i, :, lanes] = normal[i * size:(i + 1) * size].astype(jnp.bfloat16)
        for other in others:
            @pl.when(holds(other, core))
            def _():
                back(c, other).start()

    take_keys(0)
    take_queries(0)
    take_shared(0)
    key_all = stack_rows([kvbuf[0, j] for j in range(last)])
    probs = weigh(0, key_all)
    take_keys(1)
    take_shared(1)
    value_all = stack_rows([kvbuf[1, j] for j in range(last)])
    attend(0, probs, value_all)
    for c in range(1, count):
        take_queries(c)
        attend(c, weigh(c, key_all), value_all)

    @pl.when(alive)
    def _():
        for c in range(count):
            for peer in reversed(peers):
                spread(c, z, peer, atts[c].at[z]).start()
            xbufs[c][bucket, z] = atts[c][z]
            for other in others:
                place = xbufs[c].at[bucket, other]
                remote(place, place, r_send.at[c, other], r_recv.at[c, other], partner).wait_recv()
                for peer in reversed(peers):
                    spread(c, other, peer, place).start()

    w_copy.wait()

    @pl.when(alive)
    def _():
        for c, (start, size) in enumerate(chunks):
            for which in [bucket] + peers:
                if which is not bucket:
                    for other in range(nz):
                        place = xbufs[c].at[which, other]
                        remote(
                            place, place, m_send.at[c, which, other], m_recv.at[c, which, other],
                            partner,
                        ).wait_recv()
                left = jnp.concatenate([xbufs[c][which, i] for i in range(nz)], axis=1)
                value = jnp.dot(
                    left, weight[...], preferred_element_type=jnp.float32
                ).astype(jnp.bfloat16)
                if which is bucket:
                    out_ref[start:start + size, columns_of(bucket)] = value
                else:
                    ybufs[c][which] = value
                    result(c, which, bucket).start()
        for c in range(count):
            for peer in peers:
                result(c, peer, peer).wait_recv()
        for c in range(count):
            for peer in peers:
                result(c, peer, bucket).wait_send()
                spread(c, z, peer, atts[c].at[z]).wait_send()
                for other in others:
                    spread(c, other, peer, xbufs[c].at[bucket, other]).wait_send()
            for other in others:
                send_queries(c, other).wait_send()
        for kind in range(2):
            for other in others:
                send_keys(kind, other).wait_send()

    for other in others:
        @pl.when(holds(other, core))
        def _():
            for c in range(count):
                back(c, other).wait_send()
    for other in range(nz):
        @pl.when(holds(other, core))
        def _():
            for kind in range(2):
                share(kind, other, core).wait_send()


def fused_shards(nb, nz, queries, keys, values, bucket_lens, gate, out_weight):
    rows, width = queries.shape[1:]
    cols = out_weight.shape[1]
    span = width // nz
    chunks = row_chunks(rows)
    count = len(chunks)
    low = jnp.bfloat16
    dma = pltpu.SemaphoreType.DMA
    anywhere = pl.BlockSpec(memory_space=pl.ANY)
    projected = pl.pallas_call(
        functools.partial(fused_kernel, nb, nz, chunks),
        out_shape=pltpu.VMEM((rows, nb * cols), low),
        in_specs=[pl.BlockSpec(memory_space=pltpu.SMEM)] + [anywhere] * 4,
        out_specs=pl.BlockSpec(memory_space=pltpu.VMEM),
        scratch_shapes=[
            pltpu.VMEM((3, rows, width), low),
            pltpu.VMEM((width, cols), low),
            pltpu.VMEM((2, nz * CORES, rows, span), low),
            dma((3,)), dma((2,)), dma,
            dma((2, nz)), dma((2, nz)),
            dma((count, nz)), dma((count, nz)),
            dma((2, nz)), dma((2, nz)),
            dma((count, nz)), dma((count, nz)),
            dma((count, nb, nz)), dma((count, nb, nz)),
            dma((count, nb)), dma((count, nb)),
        ]
        + [pltpu.VMEM((nz, size, span), low) for _, size in chunks]
        + [pltpu.VMEM((nz, size, span), low) for _, size in chunks]
        + [pltpu.VMEM((nb, nz, size, span), low) for _, size in chunks]
        + [pltpu.VMEM((nb, size, cols), low) for _, size in chunks],
        compiler_params=pltpu.CompilerParams(collective_id=0, has_side_effects=True),
    )(bucket_lens, queries, keys, values, out_weight)
    position = lax.axis_index("seq") * rows + lax.iota(jnp.int32, rows)
    gated = projected.astype(jnp.float32) * gate[0][None, :]
    keep = (position < bucket_lens[0])[:, None]
    return jnp.where(keep, gated, 0.0).astype(jnp.bfloat16)[None]


def solution(mesh):
    placed = (
        P("bucket", "seq", None),
        P("bucket", "seq", None),
        P("bucket", "seq", None),
        P("bucket"),
        P("bucket", None),
        P(None, "bucket"),
    )
    nb, ns = mesh.shape["bucket"], mesh.shape["seq"]
    body = shards
    if ns % CORES == 0 and HEADS % (ns // CORES) == 0:
        body = functools.partial(fused_shards, nb, ns // CORES)
    return jax.shard_map(
        body, mesh=mesh, in_specs=placed, out_specs=P("bucket", "seq", None), check_vma=False
    )
```

```python
import functools

import jax
import jax.numpy as jnp
from jax import lax
from jax.experimental import pallas as pl
from jax.experimental.pallas import tpu as pltpu
from jax.sharding import PartitionSpec as P

HEADS = 12
HEAD_DIM = 128
CORES = 2
CHUNKS = 2

NEG_FILL = -1e30


def block_stats(queries, keys, values, usable):
    scores = jnp.einsum(
        "qhe,nkhe->nhqk", queries, keys, preferred_element_type=jnp.float32
    ) * HEAD_DIM ** (-0.5)
    keep_mask = usable[:, None, None, :]
    scores = jnp.where(keep_mask, scores, NEG_FILL)
    maxima = jnp.max(scores, axis=3)
    weights = jnp.where(keep_mask, jnp.exp(scores - maxima[..., None]), 0.0)
    totals = jnp.sum(weights, axis=3)
    weighted = jnp.einsum(
        "nhqk,nkhe->nqhe", weights.astype(jnp.bfloat16), values, preferred_element_type=jnp.float32
    )
    divisor = jnp.transpose(jnp.maximum(totals, 1.0), (0, 2, 1))
    partial_value = (weighted / divisor[..., None]).astype(jnp.bfloat16)
    return (partial_value, jnp.transpose(maxima, (0, 2, 1)), jnp.transpose(totals, (0, 2, 1)))


def combine(partial_value, maxima, totals):
    row_max = jnp.max(maxima, axis=0)
    factors = totals * jnp.exp(maxima - row_max[None])
    summed = jnp.einsum("nqh,nqhe->qhe", factors, partial_value.astype(jnp.float32))
    attended = summed / jnp.sum(factors, axis=0)[..., None]
    return attended.reshape(attended.shape[0], -1).astype(jnp.bfloat16)


def shards(queries, keys, values, bucket_lens, gate, out_weight):
    rows_here = queries.shape[1]
    width = queries.shape[2]
    length = bucket_lens[0]
    position = lax.axis_index("seq") * rows_here + lax.iota(jnp.int32, rows_here)
    queries_all = lax.all_gather(queries[0], "seq", axis=0, tiled=True)
    count_all = queries_all.shape[0]
    key_usable = (position < length)[None, :]
    partial_value, maxima, totals = block_stats(
        queries_all.reshape(count_all, HEADS, HEAD_DIM),
        keys[0].reshape(1, rows_here, HEADS, HEAD_DIM),
        values[0].reshape(1, rows_here, HEADS, HEAD_DIM),
        key_usable,
    )
    block_max, block_total = (
        lax.all_to_all(maxima, "seq", split_axis=1, concat_axis=0, tiled=True),
        lax.all_to_all(totals, "seq", split_axis=1, concat_axis=0, tiled=True),
    )
    block_part = lax.all_to_all(
        partial_value.reshape(1, count_all, width), "seq", split_axis=1, concat_axis=0, tiled=True
    )
    shaped = block_part.reshape(block_part.shape[0], block_part.shape[1], HEADS, HEAD_DIM)
    attended = combine(shaped, block_max, block_total)
    gate_row = gate[0]
    projected = (
        jnp.dot(
            attended,
            lax.all_gather(out_weight, "bucket", axis=1, tiled=True),
            preferred_element_type=jnp.float32,
        )
        * gate_row[None, :]
    )
    result = jnp.where((position < length)[:, None], projected, 0.0).astype(jnp.bfloat16)
    return result[None]


def remote(src, dst, send, recv, where):
    return pltpu.make_async_remote_copy(
        src_ref=src, dst_ref=dst, send_sem=send, recv_sem=recv,
        device_id=where, device_id_type=pl.DeviceIdType.MESH,
    )


def stack_rows(blocks):
    wide = jnp.concatenate([block.astype(jnp.float32) for block in blocks], axis=0)
    return wide.astype(jnp.bfloat16)


def row_chunks(rows):
    if CHUNKS == 1 or rows % 8 != 0 or rows < 32:
        return [(0, rows)]
    head = (rows // 2 + 15) // 16 * 16
    return [(0, head), (head, rows - head)]


def fused_kernel(nb, nz, chunks, len_ref, q_hbm, k_hbm, v_hbm, w_hbm, out_ref, *refs):
    (
        own, weight, kvbuf, load_sem, slot_sem, w_sem, a_send, a_recv, q_send, q_recv,
        c_send, c_recv, r_send, r_recv, m_send, m_recv, y_send, y_recv,
    ) = refs[:18]
    count = len(chunks)
    qbufs, atts, xbufs, ybufs = [refs[18 + n * count:18 + (n + 1) * count] for n in range(4)]
    _, _, rows, span = kvbuf.shape
    cols = weight.shape[1]
    bucket = lax.axis_index("bucket")
    seq = lax.axis_index("seq")
    z = seq // CORES
    core = lax.rem(seq, CORES)
    last = nz * CORES - 1
    alive = seq < last
    steps = list(range(2, nz - 1)) + [1, nz - 1] if nz > 2 else list(range(1, nz))
    others = [lax.rem(z + step, nz) for step in steps]
    peers = [lax.rem(bucket + step, nb) for step in range(1, nb)]
    if nb & (nb - 1) == 0:
        peers = [lax.bitwise_xor(bucket, step) for step in range(1, nb)]
    partner = (bucket, z * CORES + (1 - core))

    def chip(other):
        return (bucket, other * CORES + core)

    def holds(other, which):
        return other * CORES + which < last

    barrier = pltpu.get_barrier_semaphore()
    friends = [chip(o) for o in reversed(others)] + [(p, seq) for p in peers] + [partner]
    for friend in friends:
        pl.semaphore_signal(
            barrier, inc=1, device_id=friend, device_id_type=pl.DeviceIdType.MESH
        )

    loads = []
    for kind, ref in ((1, k_hbm), (0, q_hbm), (2, v_hbm)):
        loads.append(pltpu.make_async_copy(ref.at[0], own.at[kind], load_sem.at[kind]))
    mine = pl.ds(pl.multiple_of(z * span, 128), span)
    for kind, ref in ((0, k_hbm), (1, v_hbm)):
        loads.append(
            pltpu.make_async_copy(ref.at[0, :, mine], kvbuf.at[kind, seq], slot_sem.at[kind])
        )
    for copy in loads:
        copy.start()
    w_copy = pltpu.make_async_copy(w_hbm, weight, w_sem)
    w_copy.start()
    for copy in loads:
        copy.wait()
    pl.semaphore_wait(barrier, len(friends))

    def lanes_of(other):
        return pl.ds(pl.multiple_of(other * span, 128), span)

    def send_keys(kind, other):
        return remote(
            own.at[1 + kind, :, lanes_of(other)], kvbuf.at[kind, seq],
            a_send.at[kind, other], a_recv.at[kind, z], chip(other),
        )

    def send_queries(c, other):
        start, size = chunks[c]
        return remote(
            own.at[0, pl.ds(start, size), lanes_of(other)], qbufs[c].at[z],
            q_send.at[c, other], q_recv.at[c, z], chip(other),
        )

    def share(kind, other, which):
        place = kvbuf.at[kind, other * CORES + which]
        return remote(
            place, place, c_send.at[kind, other], c_recv.at[kind, other], partner
        )

    def back(c, other):
        return remote(
            atts[c].at[other], xbufs[c].at[bucket, z], r_send.at[c, other], r_recv.at[c, z],
            chip(other),
        )

    def spread(c, other, peer, source):
        return remote(
            source, xbufs[c].at[bucket, other],
            m_send.at[c, peer, other], m_recv.at[c, bucket, other], (peer, seq),
        )

    def columns_of(which):
        return pl.ds(pl.multiple_of(which * cols, 128), cols)

    def result(c, peer, which):
        place = out_ref.at[pl.ds(*chunks[c]), columns_of(which)]
        return remote(
            ybufs[c].at[peer], place, y_send.at[c, peer], y_recv.at[c, which], (peer, seq)
        )

    @pl.when(alive)
    def _():
        for other in others:
            send_keys(0, other).start()
        for other in others:
            send_queries(0, other).start()
        for other in others:
            send_keys(1, other).start()
        for c in range(1, count):
            for other in others:
                send_queries(c, other).start()
        share(0, z, core).start()
        share(1, z, core).start()

    for c, (start, size) in enumerate(chunks):
        qbufs[c][z] = own[0, start:start + size, mine]

    def take_keys(kind):
        for other in others:
            @pl.when(holds(other, core))
            def _():
                place = kvbuf.at[kind, other * CORES + core]
                remote(
                    place, place, a_send.at[kind, other], a_recv.at[kind, other], partner
                ).wait_recv()
                share(kind, other, core).start()

    def take_shared(kind):
        for other in range(nz):
            @pl.when(holds(other, 1 - core))
            def _():
                share(kind, other, 1 - core).wait_recv()

    def take_queries(c):
        for other in others:
            @pl.when(holds(other, core))
            def _():
                place = qbufs[c].at[other]
                remote(
                    place, place, q_send.at[c, other], q_recv.at[c, other], partner
                ).wait_recv()

    length = len_ref[0]
    heads = [slice(h * HEAD_DIM, (h + 1) * HEAD_DIM) for h in range(span // HEAD_DIM)]

    def weigh(c, key_all):
        size = chunks[c][1]
        query_all = stack_rows([qbufs[c][i] for i in range(nz)])
        usable = lax.broadcasted_iota(jnp.int32, (last * rows, nz * size), 0) < length
        probs = []
        for lanes in heads:
            scores = lax.dot_general(
                key_all[:, lanes], query_all[:, lanes], (((1,), (1,)), ((), ())),
                preferred_element_type=jnp.float32,
            ) * HEAD_DIM ** (-0.5)
            scores = jnp.where(usable, scores, NEG_FILL)
            top = jnp.max(scores, axis=0, keepdims=True)
            prob = jnp.exp(scores - top)
            probs.append((prob.astype(jnp.bfloat16), jnp.sum(prob, axis=0, keepdims=True)))
        return probs

    def attend(c, probs, value_all):
        start, size = chunks[c]
        lane = lax.broadcasted_iota(jnp.int32, (1, nz * size), 1)
        block = lane // size
        token = (block * CORES + core) * rows + start + (lane - block * size)
        for lanes, (prob, total) in zip(heads, probs):
            summed = lax.dot_general(
                value_all[:, lanes], prob, (((0,), (0,)), ((), ())),
                preferred_element_type=jnp.float32,
            )
            normal = jnp.where(token < length, summed / total, 0.0).T
            for i in range(nz):
                atts[c][i, :, lanes] = normal[i * size:(i + 1) * size].astype(jnp.bfloat16)
        for other in others:
            @pl.when(holds(other, core))
            def _():
                back(c, other).start()

        @pl.when(alive)
        def _():
            for peer in peers:
                spread(c, z, peer, atts[c].at[z]).start()
            xbufs[c][bucket, z] = atts[c][z]

    take_keys(0)
    take_queries(0)
    take_shared(0)
    key_all = stack_rows([kvbuf[0, j] for j in range(last)])
    probs = weigh(0, key_all)
    take_keys(1)
    take_shared(1)
    value_all = stack_rows([kvbuf[1, j] for j in range(last)])
    attend(0, probs, value_all)
    for c in range(1, count):
        take_queries(c)
        attend(c, weigh(c, key_all), value_all)

    @pl.when(alive)
    def _():
        for c in range(count):
            for other in others:
                place = xbufs[c].at[bucket, other]
                remote(place, place, r_send.at[c, other], r_recv.at[c, other], partner).wait_recv()
                for peer in peers:
                    spread(c, other, peer, place).start()

    w_copy.wait()

    @pl.when(alive)
    def _():
        for c, (start, size) in enumerate(chunks):
            for which in [bucket] + peers:
                if which is not bucket:
                    for other in range(nz):
                        place = xbufs[c].at[which, other]
                        remote(
                            place, place, m_send.at[c, which, other], m_recv.at[c, which, other],
                            partner,
                        ).wait_recv()
                left = jnp.concatenate([xbufs[c][which, i] for i in range(nz)], axis=1)
                value = jnp.dot(
                    left, weight[...], preferred_element_type=jnp.float32
                ).astype(jnp.bfloat16)
                if which is bucket:
                    out_ref[start:start + size, columns_of(bucket)] = value
                else:
                    ybufs[c][which] = value
                    result(c, which, bucket).start()
        for c in range(count):
            for peer in peers:
                result(c, peer, peer).wait_recv()
        for c in range(count):
            for peer in peers:
                result(c, peer, bucket).wait_send()
                spread(c, z, peer, atts[c].at[z]).wait_send()
                for other in others:
                    spread(c, other, peer, xbufs[c].at[bucket, other]).wait_send()
            for other in others:
                send_queries(c, other).wait_send()
        for kind in range(2):
            for other in others:
                send_keys(kind, other).wait_send()

    for other in others:
        @pl.when(holds(other, core))
        def _():
            for c in range(count):
                back(c, other).wait_send()
    for other in range(nz):
        @pl.when(holds(other, core))
        def _():
            for kind in range(2):
                share(kind, other, core).wait_send()


def fused_shards(nb, nz, queries, keys, values, bucket_lens, gate, out_weight):
    rows, width = queries.shape[1:]
    cols = out_weight.shape[1]
    span = width // nz
    chunks = row_chunks(rows)
    count = len(chunks)
    low = jnp.bfloat16
    dma = pltpu.SemaphoreType.DMA
    anywhere = pl.BlockSpec(memory_space=pl.ANY)
    projected = pl.pallas_call(
        functools.partial(fused_kernel, nb, nz, chunks),
        out_shape=pltpu.VMEM((rows, nb * cols), low),
        in_specs=[pl.BlockSpec(memory_space=pltpu.SMEM)] + [anywhere] * 4,
        out_specs=pl.BlockSpec(memory_space=pltpu.VMEM),
        scratch_shapes=[
            pltpu.VMEM((3, rows, width), low),
            pltpu.VMEM((width, cols), low),
            pltpu.VMEM((2, nz * CORES, rows, span), low),
            dma((3,)), dma((2,)), dma,
            dma((2, nz)), dma((2, nz)),
            dma((count, nz)), dma((count, nz)),
            dma((2, nz)), dma((2, nz)),
            dma((count, nz)), dma((count, nz)),
            dma((count, nb, nz)), dma((count, nb, nz)),
            dma((count, nb)), dma((count, nb)),
        ]
        + [pltpu.VMEM((nz, size, span), low) for _, size in chunks]
        + [pltpu.VMEM((nz, size, span), low) for _, size in chunks]
        + [pltpu.VMEM((nb, nz, size, span), low) for _, size in chunks]
        + [pltpu.VMEM((nb, size, cols), low) for _, size in chunks],
        compiler_params=pltpu.CompilerParams(collective_id=0, has_side_effects=True),
    )(bucket_lens, queries, keys, values, out_weight)
    position = lax.axis_index("seq") * rows + lax.iota(jnp.int32, rows)
    gated = projected.astype(jnp.float32) * gate[0][None, :]
    keep = (position < bucket_lens[0])[:, None]
    return jnp.where(keep, gated, 0.0).astype(jnp.bfloat16)[None]


def solution(mesh):
    placed = (
        P("bucket", "seq", None),
        P("bucket", "seq", None),
        P("bucket", "seq", None),
        P("bucket"),
        P("bucket", None),
        P(None, "bucket"),
    )
    nb, ns = mesh.shape["bucket"], mesh.shape["seq"]
    body = shards
    if ns % CORES == 0 and HEADS % (ns // CORES) == 0:
        body = functools.partial(fused_shards, nb, ns // CORES)
    return jax.shard_map(
        body, mesh=mesh, in_specs=placed, out_specs=P("bucket", "seq", None), check_vma=False
    )
```
